32 devices in a mesh: layer: 8 (over z, x), rep: 4 (over y, core).
Axes of the slice: x: 2, y: 2, z: 4, core: 2. Of those that a mesh axis runs over, the one named last changes fastest.
Arguments:
- inverse_root: bfloat16 [64, 16, 128, 128], P('layer', 'rep'), may hold values from -0.625 to 0.625
- square_root: bfloat16 [64, 16, 128, 128], P('layer', 'rep'), may hold values from -0.625 to 0.625
- pattern: int32 [64, 16], P('layer', 'rep'), may hold values from 0 to 1, as said below
Outputs:
- inverse_next: bfloat16 [64, 16, 128, 128], P('layer', 'rep')
- square_next: bfloat16 [64, 16, 128, 128], P('layer', 'rep')
The draws below stay inside these ranges and needn't reach their ends.
Inputs may be any that keep to these rules, and one draw needn't show every extreme that they name: 1 marks a tile of the common pattern. Slot 8 is 1 in every block row, and slot w of block row i is 0 where i - 8 + w lies outside 0 to 63.
All inputs are finite; a program needn't handle non-finite values.
Results may differ from the reference program's by a relative error of at most 0.018.
Values may be sent and summed in bfloat16 or wider, within the bound.
No kernel may reach another device: no remote copies, remote signals or barrier semaphores. Data moves between devices by JAX's collectives and lax.ppermute only.
A program may use at most 128 MiB of HBM per device.

```python
import jax
import jax.numpy as jnp
from jax import lax

TILE = 128
BAND = 16
HALF = 8
NB = 64
N_REP = 4


def draw_pattern(key, part):
    row_ids = jnp.arange(NB, dtype=jnp.int32)[:, None]
    slot_ids = jnp.arange(BAND, dtype=jnp.int32)[None, :]
    column = row_ids - HALF + slot_ids
    inside = (column >= 0) & (column < NB)
    key_level = jax.random.fold_in(key, 11)
    key_tiles = jax.random.fold_in(key, 23)
    fill_level = jax.random.randint(key_level, (NB, 1), 15, 90)
    tile_draws = jax.random.randint(key_tiles, (NB, BAND), 0, 100)
    chosen = (tile_draws < fill_level) | (slot_ids == HALF)
    return (inside & chosen).astype(jnp.int32)


def shard_levels(own_key, shape, shards, low, high):
    def one(position, shards_of):
        draws = jax.random.uniform(jax.random.fold_in(jax.random.fold_in(own_key, 6), position), (shards_of,), jnp.float32, low / len(shards), high / len(shards))
        return jnp.repeat(jnp.exp(draws), shape[position] // shards_of).reshape((-1,) + (1,) * (len(shape) - position - 1))

    level = one(*shards[0])
    for cut in shards[1:]:
        level = level * one(*cut)
    return level


def bell_draw(rng, shape, width, bound, pieces=(), kind=jnp.bfloat16):
    factor_of = shard_levels(rng, shape, pieces, -0.22, 0.18) if pieces else 1.0
    drawn = jax.random.normal(rng, shape, jnp.float32) * width * factor_of
    return jnp.minimum(jnp.maximum(drawn, -bound), bound).astype(kind)


def setup_inputs(seed: int = 0) -> dict:
    streams_of = jax.random.split(jax.random.key(seed), 4)
    return {
        "inverse_root": bell_draw(streams_of[0], (NB, BAND, TILE, TILE), 0.1, 0.625, ((0, 8), (1, 4))),
        "square_root": bell_draw(streams_of[1], (NB, BAND, TILE, TILE), 0.1, 0.625, ((0, 8), (1, 4))),
        "pattern": draw_pattern(jax.random.fold_in(streams_of[3], 71), 0),
    }


def band_product(left_tiles, right_tiles):
    block_rows = left_tiles.shape[0]
    band_slots = left_tiles.shape[1]
    half_band = band_slots // 2
    group_slots = band_slots // N_REP
    padded = jnp.pad(right_tiles, ((half_band, half_band), (band_slots, band_slots), (0, 0), (0, 0)))
    total = jnp.zeros(left_tiles.shape, jnp.float32)
    for group in range(N_REP):
        partial_value = jnp.zeros(left_tiles.shape, jnp.float32)
        for inner in range(group * group_slots, (group + 1) * group_slots):
            low_slot = max(0, inner - half_band)
            high_slot = min(band_slots, inner + half_band)
            offset = band_slots + half_band - inner
            shifted = padded[inner:inner + block_rows, offset + low_slot:offset + high_slot]
            product = jnp.einsum("iab,iwbc->iwac", left_tiles[:, inner].astype(jnp.float32), shifted.astype(jnp.float32))
            partial_value = partial_value.at[:, low_slot:high_slot].add(product)
        rounded = lax.optimization_barrier(partial_value.astype(jnp.bfloat16))
        total = total + rounded.astype(jnp.float32)
    return total


def reference(inverse_root, square_root, pattern):
    in_pattern = (pattern == 1)[:, :, None, None]
    inverse_kept = jnp.where(in_pattern, inverse_root, jnp.zeros_like(inverse_root))
    square_kept = jnp.where(in_pattern, square_root, jnp.zeros_like(square_root))
    intersection = jnp.where(in_pattern, band_product(inverse_kept, square_kept), jnp.float32(0.0))
    band_slots = pattern.shape[1]
    half_band = band_slots // 2
    diagonal = (jnp.arange(band_slots, dtype=jnp.int32) == half_band).astype(jnp.float32)
    identity = jnp.eye(inverse_root.shape[2], dtype=jnp.float32)
    update = jnp.where(in_pattern, 1.5 * diagonal[None, :, None, None] * identity - 0.5 * intersection, jnp.float32(0.0)).astype(jnp.bfloat16)
    square_next = jnp.where(in_pattern, band_product(square_kept, update), jnp.float32(0.0)).astype(jnp.bfloat16)
    inverse_next = jnp.where(in_pattern, band_product(update, inverse_kept), jnp.float32(0.0)).astype(jnp.bfloat16)
    return inverse_next, square_next
```

```python
import functools

import jax
import jax.numpy as jnp
from jax import lax
from jax.experimental import pallas as pl
from jax.experimental.pallas import tpu as pltpu
from jax.sharding import PartitionSpec as P


def rep_route(block, target_of):
    count = lax.axis_size("rep")
    return lax.ppermute(block, "rep", [(r, target_of(r)) for r in range(count)])


def half_swap(block):
    count = lax.axis_size("rep")
    return rep_route(block, lambda r: (r + count // 2) % count)


def group_parts(block):
    group = lax.axis_size("rep") // 2

    def back(distance):
        return lambda r: r // group * group + (r % group - distance) % group

    return [block] + [rep_route(block, back(d)) for d in range(1, group)]


def halo_shift(block):
    layers = lax.axis_size("layer")
    count = lax.axis_size("rep")
    route = []
    for layer in range(layers):
        for r in range(count):
            target = layer + 1 if r < count // 2 else layer - 1
            if 0 <= target < layers:
                route.append((layer * count + r, target * count + r))
    return lax.ppermute(block, ("layer", "rep"), route)


def product_kernel(place_ref, *refs, rows, slots, group, tile):
    left = refs[:group]
    own = [refs[group + e * group : group + (e + 1) * group] for e in range(2)]
    halo = [refs[3 * group + e * group : 3 * group + (e + 1) * group] for e in range(2)]
    kept_ref, sent_ref, left_win, right_win, sems = refs[5 * group :]
    half_band = slots * group
    half = place_ref[0]
    member = place_ref[1]
    copies = []
    for d in range(group):
        lane = lax.rem(member + d, group) * slots
        copies.append((left[d], left_win.at[:, pl.ds(lane, slots)]))
        for e in range(2):
            part_half = half if e == 0 else 1 - half
            slot = (part_half + half) * half_band + lane
            copies.append((own[e][d], right_win.at[pl.ds((1 - half) * rows, rows), pl.ds(slot, slots)]))
            copies.append((halo[e][d], right_win.at[pl.ds(half * rows, rows), pl.ds(slot, slots)]))
    copies = [pltpu.make_async_copy(src, dst, sems.at[n]) for n, (src, dst) in enumerate(copies)]
    for copy in copies:
        copy.start()
    empty = (1 - half) * 2 * half_band

    def clear(row, carry):
        right_win[row, pl.ds(empty, half_band)] = jnp.zeros((half_band, tile, tile), right_win.dtype)
        return carry

    lax.fori_loop(0, 2 * rows, clear, 0)
    for copy in copies:
        copy.wait()
    wide = 2 if slots % 2 == 0 else 1
    deep = 2 if half_band % 2 == 0 else 1

    def one_row(row, carry):
        for e in range(2):
            part_half = half if e == 0 else 1 - half
            base = part_half * half_band + member * slots + half_band
            out_ref = kept_ref if e == 0 else sent_ref
            for s in range(0, slots, wide):
                total = jnp.zeros((tile, wide * tile), jnp.float32)
                for t in range(0, half_band, deep):
                    a = jnp.concatenate([left_win[row, t + q] for q in range(deep)], axis=1)
                    b = jnp.concatenate(
                        [
                            jnp.concatenate(
                                [right_win[row + t + q, base + (s + p - t - q)] for p in range(wide)], axis=1
                            )
                            for q in range(deep)
                        ],
                        axis=0,
                    )
                    total = total + jnp.dot(a, b, preferred_element_type=jnp.float32)
                for p in range(wide):
                    out_ref[row, s + p] = total[:, p * tile : (p + 1) * tile].astype(out_ref.dtype)
        return carry

    lax.fori_loop(0, rows, one_row, 0)


def partial_products(place, left, own, halo):
    group = len(left)
    rows, slots, tile = left[0].shape[0], left[0].shape[1], left[0].shape[2]
    half_band = slots * group
    operands = list(left) + own[0] + own[1] + halo[0] + halo[1]
    out = jax.ShapeDtypeStruct((rows, slots, tile, tile), jnp.bfloat16)
    return pl.pallas_call(
        functools.partial(product_kernel, rows=rows, slots=slots, group=group, tile=tile),
        out_shape=(out, out),
        in_specs=[pl.BlockSpec(memory_space=pltpu.SMEM)]
        + [pl.BlockSpec(memory_space=pltpu.HBM)] * len(operands),
        out_specs=(pl.BlockSpec(memory_space=pltpu.VMEM), pl.BlockSpec(memory_space=pltpu.VMEM)),
        scratch_shapes=[
            pltpu.VMEM((rows, half_band, tile, tile), jnp.bfloat16),
            pltpu.VMEM((2 * rows, 3 * half_band, tile, tile), jnp.bfloat16),
            pltpu.SemaphoreType.DMA((len(operands),)),
        ],
        compiler_params=pltpu.CompilerParams(vmem_limit_bytes=40 * 1024 * 1024),
    )(place, *operands)


def body(inverse_root, square_root, pattern):
    rows, slots = pattern.shape
    count = lax.axis_size("rep")
    group = count // 2
    half_band = slots * group
    assert rows == half_band and count % 2 == 0
    replica = lax.axis_index("rep")
    place = jnp.stack([replica // group, replica % group]).astype(jnp.int32)
    in_pattern = (pattern == 1)[:, :, None, None]
    square_kept = jnp.where(in_pattern, square_root, jnp.zeros_like(square_root))
    inverse_kept = jnp.where(in_pattern, inverse_root, jnp.zeros_like(inverse_root))

    def spread(block):
        other = half_swap(block)
        pair = [block, other]
        halo = [halo_shift(block), halo_shift(other)]
        return [group_parts(p) for p in pair], [group_parts(p) for p in halo]

    def product(left, right):
        kept, sent = partial_products(place, left, *right)
        return kept.astype(jnp.float32) + half_swap(sent).astype(jnp.float32)

    square_right = spread(square_kept)
    inverse_right = spread(inverse_kept)
    intersection = product(inverse_right[0][0], square_right)
    slot_ids = replica * slots + jnp.arange(slots, dtype=jnp.int32)
    diagonal = (slot_ids == half_band).astype(jnp.float32)
    identity = jnp.eye(inverse_root.shape[2], dtype=jnp.float32)
    update = jnp.where(
        in_pattern,
        1.5 * diagonal[None, :, None, None] * identity - 0.5 * intersection,
        jnp.float32(0.0),
    ).astype(jnp.bfloat16)
    update_right = spread(update)
    inverse_next = jnp.where(in_pattern, product(update_right[0][0], inverse_right), 0.0)
    square_next = jnp.where(in_pattern, product(square_right[0][0], update_right), 0.0)
    return (inverse_next.astype(jnp.bfloat16), square_next.astype(jnp.bfloat16))


def solution(mesh):
    placed = (P("layer", "rep", None, None), P("layer", "rep", None, None), P("layer", "rep"))
    return jax.shard_map(
        body,
        mesh=mesh,
        in_specs=placed,
        out_specs=(P("layer", "rep", None, None), P("layer", "rep", None, None)),
        check_vma=False,
    )
```
